32 devices in a mesh: ty: 4 (over y, x), tx: 8 (over z, core).
Axes of the slice: x: 2, y: 2, z: 4, core: 2. Of those that a mesh axis runs over, the one named last changes fastest.
Arguments:
- surface_levels: float32 [512, 16384], P('ty', 'tx'), may hold values from -6 to 6
- bearing_index: int32 [4], replicated, may hold values from 0 to 15
- stencil_displacements: int32 [4], replicated, may hold values from -4 to 4
- camera_altitude_class: int32 [4], replicated, may hold values from 0 to 3
Outputs:
- margin: float32 [4, 512, 16384], P(None, 'ty', 'tx')
The draws below stay inside these ranges and needn't reach their ends.
Inputs may be any that keep to these rules, and one draw needn't show every extreme that they name: `bearing_index`: azimuth indices.
All inputs are finite; a program needn't handle non-finite values.
Results may differ from the reference program's by a relative error of at most 0.00002.
Values sent between devices are 32-bit elements; how exact they have to be, the bound alone decides.
No kernel may reach another device: no remote copies, remote signals or barrier semaphores. Data moves between devices by JAX's collectives and lax.ppermute only.
A program may use at most 192 MiB of HBM per device.

```python
import math
import jax
import jax.numpy as jnp
from jax import lax

AZIMUTHS = 4
STENCIL_REACH = 4
GRID_LENGTH = 512
GRID_WIDTH = 16384


def place_ends(result, stream_key, least, top_value):
    spot = [jax.random.randint(jax.random.fold_in(stream_key, axis), (), 0, length) for axis, length in enumerate(result.shape)]
    widest = result.shape.index(max(result.shape))
    beside = spot[:widest] + [(spot[widest] + 1) % result.shape[widest]] + spot[widest + 1:]
    return result.at[tuple(spot)].set(least).at[tuple(beside)].set(top_value)


def block_scale(stream_key, shape, shards, least, top_value):
    level = 1.0
    for axis_at, shards_of in shards:
        draws = jax.random.uniform(jax.random.fold_in(jax.random.fold_in(stream_key, 6), axis_at), (shards_of,), jnp.float32, least / len(shards), top_value / len(shards))
        level = level * jnp.repeat(jnp.exp(draws), shape[axis_at] // shards_of).reshape((-1,) + (1,) * (len(shape) - 1 - axis_at))
    return level


def scatter_about(own_key, dims, width, bound, pieces=(), held_as=jnp.bfloat16):
    result = width * jax.random.normal(own_key, dims, jnp.float32)
    if pieces:
        result = result * block_scale(own_key, dims, pieces, -0.22, 0.18)
    return jnp.clip(result, -bound, bound).astype(held_as)


def setup_inputs(seed: int = 0) -> dict:
    key_list = jax.random.split(jax.random.key(seed), 5)
    surface_levels = scatter_about(key_list[0], (GRID_LENGTH, GRID_WIDTH), 1.0, 6.0, ((0, 4), (1, 8)), jnp.float32)
    bearing_index = place_ends(jax.random.randint(key_list[1], (AZIMUTHS,), 0, 16), jax.random.fold_in(key_list[1], 1), 0, 15).astype(jnp.int32)
    stencil_displacements = place_ends(jax.random.randint(key_list[2], (AZIMUTHS,), -STENCIL_REACH, STENCIL_REACH + 1), jax.random.fold_in(key_list[2], 1), -STENCIL_REACH, STENCIL_REACH).astype(jnp.int32)
    camera_altitude_class = place_ends(jax.random.randint(key_list[3], (AZIMUTHS,), 0, 4), jax.random.fold_in(key_list[3], 1), 0, 3).astype(jnp.int32)
    return {"surface_levels": surface_levels, "bearing_index": bearing_index, "stencil_displacements": stencil_displacements, "camera_altitude_class": camera_altitude_class}


def view_tables(bearing_index, camera_altitude_class, easting_span):
    angle_idx = bearing_index.astype(jnp.float32)
    frac = (((bearing_index * 5) % 16).astype(jnp.float32) + 0.5) / 16.0
    theta = (angle_idx - 7.5) * (math.pi / 32.0)
    stride = 1.0 / jnp.cos(theta)
    slope = (1.0 + camera_altitude_class.astype(jnp.float32)) / (4.0 * easting_span)
    cube = frac * frac * frac
    square = frac * frac
    weights = jnp.stack([(-cube + 2.0 * square - frac) / 2.0, (3.0 * cube - 5.0 * square + 2.0) / 2.0, (-3.0 * cube + 4.0 * square + frac) / 2.0, (cube - square) / 2.0], axis=1)
    return weights, stride * slope


def reference(surface_levels, bearing_index, stencil_displacements, camera_altitude_class):
    northing_extent, easting_span = surface_levels.shape
    weights, rise = view_tables(bearing_index, camera_altitude_class, easting_span)
    border_lines = STENCIL_REACH + 2
    bordered_surface = jnp.pad(surface_levels, ((border_lines, border_lines), (0, 0)))
    columns = jnp.arange(easting_span).astype(jnp.float32)
    outputs = []
    for which in range(AZIMUTHS):
        strips = jnp.zeros((northing_extent, easting_span), jnp.float32)
        for tap_index in range(4):
            start = (stencil_displacements[which] + tap_index + STENCIL_REACH + 1).astype(jnp.int32)
            strips = strips + weights[which, tap_index] * lax.dynamic_slice_in_dim(bordered_surface, start, northing_extent, 0)
        lifted = strips + rise[which] * columns[None, :]
        running = lax.cummax(lifted, axis=1)
        lowest = jnp.full((northing_extent, 1), -jnp.inf, jnp.float32)
        horizon = jnp.concatenate([lowest, running[:, :-1]], axis=1)
        outputs.append(jnp.maximum(horizon - lifted, 0.0))
    return jnp.stack(outputs, axis=0)
```

```python
import functools
import math

import jax
import jax.numpy as jnp
from jax import lax
from jax.experimental import pallas as pl
from jax.experimental.pallas import tpu as pltpu
from jax.sharding import PartitionSpec as P

TAPS = 4
SUB = 8
LANE = 128
MIB = 1 << 20


def view_terms(bearing_ref, class_ref, which, easting_span):
    bearing = bearing_ref[which]
    frac = (lax.rem(bearing * 5, 16).astype(jnp.float32) + 0.5) * 0.0625
    theta = (bearing.astype(jnp.float32) - 7.5) * (math.pi / 32.0)
    stride = 1.0 / jnp.cos(jnp.full((SUB, LANE), theta, jnp.float32))
    slope = (1.0 + class_ref[which].astype(jnp.float32)) * (1.0 / (4.0 * easting_span))
    cube = frac * frac * frac
    square = frac * frac
    weights = (
        (-cube + 2.0 * square - frac) * 0.5,
        (3.0 * cube - 5.0 * square + 2.0) * 0.5,
        (-3.0 * cube + 4.0 * square + frac) * 0.5,
        (cube - square) * 0.5,
    )
    return weights, stride * slope


def column_tile(first_col, block):
    lane = lax.broadcasted_iota(jnp.int32, (SUB, LANE), 1)
    return (lane + (first_col + block * LANE)).astype(jnp.float32)


def lifted_tile(weights, ramp, rows_at):
    total = weights[0] * rows_at(0)
    for tap in range(1, TAPS):
        total = total + weights[tap] * rows_at(tap)
    return total + ramp


def scan_tiles(source, work, blocks):
    lane = lax.broadcasted_iota(jnp.int32, (SUB, LANE), 1)
    tiles = source
    step = 1
    while step < LANE:
        mask = lane < step
        for get, put in tiles(step):
            values = [get(j) for j in range(blocks)]
            rolled = [pltpu.roll(v, step, 1) for v in values]
            for j in range(blocks):
                before = rolled[j - 1] if j else jnp.full((SUB, LANE), -jnp.inf, jnp.float32)
                put(j, jnp.maximum(values[j], jnp.where(mask, before, rolled[j])))
        step *= 2


def inner_kernel(bearing_ref, disp_ref, class_ref, x_ref, lifted_ref, margin_ref, edge_ref, peak_ref, own, work, sems, *, tx):
    rows, cols = x_ref.shape
    blocks, tiles = cols // LANE, rows // SUB
    views = bearing_ref.shape[0]
    copies = [
        pltpu.make_async_copy(x_ref.at[:, pl.ds(j * LANE, LANE)], own.at[j], sems.at[j])
        for j in range(blocks)
    ]
    for copy in copies:
        copy.start()
    first_col = lax.axis_index("tx") * cols
    terms = [view_terms(bearing_ref, class_ref, k, cols * tx) for k in range(views)]
    for copy in copies:
        copy.wait()
    for j in range(blocks):
        edge_ref[0, j] = own[j, 0 : 2 * SUB, :]
        edge_ref[1, j] = own[j, rows - 2 * SUB : rows, :]
    for which in range(views):
        weights, rise = terms[which]
        disp = disp_ref[which] - 1
        ramps = [rise * column_tile(first_col, j) for j in range(blocks)]

        @pl.loop(1, tiles - 1)
        def _(t):
            for j in range(blocks):
                lifted_ref[which, t, j] = lifted_tile(
                    weights, ramps[j], lambda tap: own[j, pl.ds(t * SUB + disp + tap, SUB), :]
                )

        def stages(step):
            for t in range(1, tiles - 1):
                yield (
                    (lambda j, t=t: lifted_ref[which, t, j]) if step == 1 else (lambda j, t=t: work[t, j]),
                    functools.partial(put_tile, work, t),
                )

        scan_tiles(stages, None, blocks)
        for t in range(1, tiles - 1):
            peak = None
            for j in range(blocks):
                peak = work[t, j] if peak is None else jnp.maximum(peak, work[t, j])
                margin_ref[which, t, j] = peak - lifted_ref[which, t, j]
            peak_ref[which, t] = peak


def put_tile(ref, t, j, value):
    ref[t, j] = value


def edge_kernel(bearing_ref, disp_ref, class_ref, up_ref, down_ref, edge_ref, peak_ref, lifted_ref, sent_ref, ring, tall, *, tx, ty):
    cols = up_ref.shape[1]
    blocks = cols // LANE
    views, tiles = peak_ref.shape[:2]
    place = lax.axis_index("ty")
    first_col = lax.axis_index("tx") * cols
    for j in range(blocks):
        span = slice(j * LANE, (j + 1) * LANE)
        ring[0, j, 0:SUB, :] = jnp.where(place == 0, 0.0, up_ref[:, span])
        ring[0, j, SUB : 3 * SUB, :] = edge_ref[0, j]
        ring[1, j, 0 : 2 * SUB, :] = edge_ref[1, j]
        ring[1, j, 2 * SUB : 3 * SUB, :] = jnp.where(place == ty - 1, 0.0, down_ref[:, span])
    for which in range(views):
        weights, rise = view_terms(bearing_ref, class_ref, which, cols * tx)
        disp = disp_ref[which] - 1
        tops = []
        for end in range(2):
            top = None
            for j in range(blocks):
                value = lifted_tile(
                    weights,
                    rise * column_tile(first_col, j),
                    lambda tap: ring[end, j, pl.ds(SUB + disp + tap, SUB), :],
                )
                lifted_ref[which, end, j] = value
                top = value if top is None else jnp.maximum(top, value)
            tops.append(top)
        tall[0:SUB, :] = tops[0]
        for t in range(1, tiles - 1):
            tall[t * SUB : (t + 1) * SUB, :] = peak_ref[which, t]
        tall[(tiles - 1) * SUB : tiles * SUB, :] = tops[1]
        peaks = jnp.max(jnp.transpose(tall[...]), axis=0, keepdims=True)
        for i in range(tx):
            sent_ref[i, which : which + 1, :] = peaks


def final_kernel(got_ref, lifted_ref, margin_ref, edge_ref, out_ref, stage, work, tall, sems, *, tx):
    views, rows, cols = out_ref.shape
    blocks, tiles = cols // LANE, rows // SUB
    place = lax.axis_index("tx")
    before = jnp.full((views, rows), -jnp.inf, jnp.float32)
    for i in range(tx):
        before = jnp.maximum(before, jnp.where(i < place, got_ref[i], -jnp.inf))
    for which in range(views):
        tall[which] = jnp.transpose(jnp.broadcast_to(before[which : which + 1, :], (LANE, rows)))
    copies = []
    for which in range(views):

        @pl.loop(1, tiles - 1)
        def _(t):
            top = tall[which, pl.ds(t * SUB, SUB), :]
            for j in range(blocks):
                stage[which, pl.ds(t * SUB, SUB), j * LANE : (j + 1) * LANE] = jnp.maximum(
                    margin_ref[which, t, j], top - lifted_ref[which, t, j]
                )

        inner = pl.ds(SUB, rows - 2 * SUB)
        copies.append(pltpu.make_async_copy(stage.at[which, inner], out_ref.at[which, inner], sems.at[which, 0]))
        copies[-1].start()

    def stages(step):
        for which in range(views):
            for end in range(2):
                at = which * 2 + end
                yield (
                    (lambda j, which=which, end=end: edge_ref[which, end, j]) if step == 1 else (lambda j, at=at: work[at, j]),
                    functools.partial(put_tile, work, at),
                )

    scan_tiles(stages, None, blocks)
    for which in range(views):
        for end in range(2):
            first = end * (rows - SUB)
            peak = tall[which, first : first + SUB, :]
            for j in range(blocks):
                peak = jnp.maximum(peak, work[which * 2 + end, j])
                stage[which, first : first + SUB, j * LANE : (j + 1) * LANE] = peak - edge_ref[which, end, j]
            outer = pl.ds(first, SUB)
            copies.append(pltpu.make_async_copy(stage.at[which, outer], out_ref.at[which, outer], sems.at[which, 1 + end]))
            copies[-1].start()
    for copy in copies:
        copy.wait()


def on_device(ty, tx, surface, bearing, disp, altitude):
    rows, cols = surface.shape
    views = bearing.shape[0]
    tiles, blocks = rows // SUB, cols // LANE
    f32 = jnp.float32
    up = lax.ppermute(surface[rows - SUB :], "ty", [(i, (i + 1) % ty) for i in range(ty)])
    down = lax.ppermute(surface[:SUB], "ty", [((i + 1) % ty, i) for i in range(ty)])
    smem = pl.BlockSpec(memory_space=pltpu.SMEM)
    vmem = pl.BlockSpec(memory_space=pltpu.VMEM)
    hbm = pl.BlockSpec(memory_space=pl.ANY)
    lifted, margin, edge, peak = pl.pallas_call(
        functools.partial(inner_kernel, tx=tx),
        out_shape=(
            pltpu.VMEM((views, tiles, blocks, SUB, LANE), f32),
            pltpu.VMEM((views, tiles, blocks, SUB, LANE), f32),
            pltpu.VMEM((2, blocks, 2 * SUB, LANE), f32),
            pltpu.VMEM((views, tiles, SUB, LANE), f32),
        ),
        in_specs=[smem, smem, smem, hbm],
        out_specs=[vmem] * 4,
        scratch_shapes=[
            pltpu.VMEM((blocks, rows, LANE), f32),
            pltpu.VMEM((tiles, blocks, SUB, LANE), f32),
            pltpu.SemaphoreType.DMA((blocks,)),
        ],
        compiler_params=pltpu.CompilerParams(vmem_limit_bytes=24 * MIB),
        cost_estimate=pl.CostEstimate(flops=views * rows * cols * 40, bytes_accessed=rows * cols * 4, transcendentals=0),
        name="inner",
    )(bearing, disp, altitude, surface)
    outer, sent = pl.pallas_call(
        functools.partial(edge_kernel, tx=tx, ty=ty),
        out_shape=(
            pltpu.VMEM((views, 2, blocks, SUB, LANE), f32),
            jax.ShapeDtypeStruct((tx, views, rows), f32),
        ),
        in_specs=[smem, smem, smem] + [vmem] * 4,
        out_specs=[vmem] * 2,
        scratch_shapes=[pltpu.VMEM((2, blocks, 3 * SUB, LANE), f32), pltpu.VMEM((rows, LANE), f32)],
        compiler_params=pltpu.CompilerParams(vmem_limit_bytes=16 * MIB),
        name="edges",
    )(bearing, disp, altitude, up, down, edge, peak)
    got = lax.all_to_all(sent, "tx", 0, 0)
    return pl.pallas_call(
        functools.partial(final_kernel, tx=tx),
        out_shape=jax.ShapeDtypeStruct((views, rows, cols), f32),
        in_specs=[vmem] * 4,
        out_specs=hbm,
        scratch_shapes=[
            pltpu.VMEM((views, rows, cols), f32),
            pltpu.VMEM((views * 2, blocks, SUB, LANE), f32),
            pltpu.VMEM((views, rows, LANE), f32),
            pltpu.SemaphoreType.DMA((views, 3)),
        ],
        compiler_params=pltpu.CompilerParams(vmem_limit_bytes=24 * MIB),
        name="finish",
    )(got, lifted, margin, outer)


def solution(mesh):
    return jax.shard_map(
        functools.partial(on_device, mesh.shape["ty"], mesh.shape["tx"]),
        mesh=mesh,
        in_specs=(P("ty", "tx"), P(), P(), P()),
        out_specs=P(None, "ty", "tx"),
        check_vma=False,
    )
```

```python
import functools
import math

import jax
import jax.numpy as jnp
from jax import lax
from jax.experimental import pallas as pl
from jax.experimental.pallas import tpu as pltpu
from jax.sharding import PartitionSpec as P

TAPS = 4
SUB = 8
LANE = 128
MIB = 1 << 20
EARLY = 1


def view_terms(bearing_ref, class_ref, which, easting_span):
    bearing = bearing_ref[which]
    frac = (lax.rem(bearing * 5, 16).astype(jnp.float32) + 0.5) * 0.0625
    theta = (bearing.astype(jnp.float32) - 7.5) * (math.pi / 32.0)
    stride = 1.0 / jnp.cos(jnp.full((SUB, LANE), theta, jnp.float32))
    slope = (1.0 + class_ref[which].astype(jnp.float32)) * (1.0 / (4.0 * easting_span))
    cube = frac * frac * frac
    square = frac * frac
    weights = (
        (-cube + 2.0 * square - frac) * 0.5,
        (3.0 * cube - 5.0 * square + 2.0) * 0.5,
        (-3.0 * cube + 4.0 * square + frac) * 0.5,
        (cube - square) * 0.5,
    )
    return weights, stride * slope


def column_tile(first_col, block):
    lane = lax.broadcasted_iota(jnp.int32, (SUB, LANE), 1)
    return (lane + (first_col + block * LANE)).astype(jnp.float32)


def lifted_tile(weights, ramp, rows_at):
    total = weights[0] * rows_at(0)
    for tap in range(1, TAPS):
        total = total + weights[tap] * rows_at(tap)
    return total + ramp


def scan_tiles(count, load, work, blocks):
    lane = lax.broadcasted_iota(jnp.int32, (SUB, LANE), 1)
    lowest = jnp.full((SUB, LANE), -jnp.inf, jnp.float32)
    step = 1
    while step < LANE:
        for t in range(count):
            values = [load(t, j) if step == 1 else work[t, j] for j in range(blocks)]
            left = lowest
            for j in range(blocks):
                here = pltpu.roll(values[j], step, 1)
                work[t, j] = jnp.maximum(values[j], jnp.where(lane < step, left, here))
                left = here
        step *= 2


def scan_view(count, load, store, work, blocks):
    scan_tiles(count, load, work, blocks)
    for t in range(count):
        peak = work[t, 0]
        store(t, 0, peak - load(t, 0))
        for j in range(1, blocks):
            peak = jnp.maximum(peak, work[t, j])
            store(t, j, peak - load(t, j))


def inner_kernel(
    bearing_hbm, disp_hbm, class_hbm, x_ref, lifted_ref, margin_ref, edge_ref, peak_ref, terms_ref, disp_out,
    own, work, bearing_ref, disp_ref, class_ref, sems, few_sems, *, tx,
):
    rows, cols = x_ref.shape
    blocks, tiles = cols // LANE, rows // SUB
    views = bearing_ref.shape[0]
    few = [
        pltpu.make_async_copy(source, target, few_sems.at[i])
        for i, (source, target) in enumerate(((bearing_hbm, bearing_ref), (disp_hbm, disp_ref), (class_hbm, class_ref)))
    ]
    for copy in few:
        copy.start()
    copies = [
        pltpu.make_async_copy(x_ref.at[:, pl.ds(j * LANE, LANE)], own.at[j], sems.at[j])
        for j in range(blocks)
    ]
    for copy in copies:
        copy.start()
    first_col = lax.axis_index("tx") * cols
    for copy in few:
        copy.wait()
    for which in range(views):
        weights, rise = view_terms(bearing_ref, class_ref, which, cols * tx)
        disp_out[which] = disp_ref[which]
        for tap in range(TAPS):
            terms_ref[which, tap] = jnp.full((SUB, LANE), weights[tap], jnp.float32)
        terms_ref[which, TAPS] = rise
        for t in range(1, tiles - 1):
            peak_ref[which, t] = jnp.full((SUB, LANE), -jnp.inf, jnp.float32)

    for copy in copies:
        copy.wait()

    @pl.loop(0, blocks)
    def _(j):
        edge_ref[0, j] = own[j, 0 : 2 * SUB, :]
        edge_ref[1, j] = own[j, rows - 2 * SUB : rows, :]
        column = column_tile(first_col, j)
        for which in range(views):
            weights = [terms_ref[which, tap] for tap in range(TAPS)]
            ramp = terms_ref[which, TAPS] * column
            disp = disp_ref[which] - 1
            for t in range(1, tiles - 1):
                value = lifted_tile(weights, ramp, lambda tap: own[j, pl.ds(t * SUB + disp + tap, SUB), :])
                lifted_ref[which, t, j] = value
                peak_ref[which, t] = jnp.maximum(peak_ref[which, t], value)

    for which in range(EARLY):
        scan_view(
            tiles - 2,
            lambda t, j: lifted_ref[which, t + 1, j],
            functools.partial(put_tile, margin_ref, which),
            work,
            blocks,
        )


def put_tile(ref, which, t, j, value):
    ref[which, t, j] = value


def edge_kernel(disp_ref, terms_ref, up_ref, down_ref, edge_ref, peak_ref, lifted_ref, sent_ref, ring, tall, *, ty):
    cols = up_ref.shape[1]
    blocks = cols // LANE
    views, tiles = peak_ref.shape[:2]
    place = lax.axis_index("ty")
    first_col = lax.axis_index("tx") * cols
    for j in range(blocks):
        span = slice(j * LANE, (j + 1) * LANE)
        ring[0, j, 0:SUB, :] = jnp.where(place == 0, 0.0, up_ref[:, span])
        ring[0, j, SUB : 3 * SUB, :] = edge_ref[0, j]
        ring[1, j, 0 : 2 * SUB, :] = edge_ref[1, j]
        ring[1, j, 2 * SUB : 3 * SUB, :] = jnp.where(place == ty - 1, 0.0, down_ref[:, span])
    for which in range(views):
        weights, rise = [terms_ref[which, tap] for tap in range(TAPS)], terms_ref[which, TAPS]
        disp = disp_ref[which] - 1
        tops = []
        for end in range(2):
            top = None
            for j in range(blocks):
                value = lifted_tile(
                    weights,
                    rise * column_tile(first_col, j),
                    lambda tap: ring[end, j, pl.ds(SUB + disp + tap, SUB), :],
                )
                lifted_ref[which, end, j] = value
                top = value if top is None else jnp.maximum(top, value)
            tops.append(top)
        tall[0:SUB, :] = tops[0]
        for t in range(1, tiles - 1):
            tall[t * SUB : (t + 1) * SUB, :] = peak_ref[which, t]
        tall[(tiles - 1) * SUB : tiles * SUB, :] = tops[1]
        sent_ref[which : which + 1, :] = jnp.max(jnp.transpose(tall[...]), axis=0, keepdims=True)


def late_kernel(lifted_ref, edge_ref, margin_ref, edge_margin_ref, work):
    views, tiles, blocks = lifted_ref.shape[:3]

    @pl.loop(EARLY, views)
    def _(which):
        scan_view(
            tiles - 2,
            lambda t, j: lifted_ref[which, t + 1, j],
            functools.partial(put_tile, margin_ref, which - EARLY),
            work,
            blocks,
        )

    scan_view(
        views * 2,
        lambda t, j: edge_ref[t // 2, t % 2, j],
        lambda t, j, value: put_tile(edge_margin_ref, t // 2, t % 2, j, value),
        work,
        blocks,
    )


def final_kernel(*refs, tx):
    partner_ref, *got_refs = refs[: tx // 2]
    lifted_ref, early_ref, late_ref, edge_ref, edge_margin_ref, out_ref, stage, tall, sems = refs[tx // 2 :]
    views, rows, cols = out_ref.shape
    blocks, tiles = cols // LANE, rows // SUB
    place = lax.axis_index("tx")
    chip = place // 2
    before = jnp.where(lax.rem(place, 2) == 1, partner_ref[...], -jnp.inf)
    for i, got_ref in enumerate(got_refs):
        before = jnp.maximum(before, jnp.where((chip ^ (i + 1)) < chip, got_ref[...], -jnp.inf))
    for which in range(views):
        tall[which] = jnp.transpose(jnp.broadcast_to(before[which : which + 1, :], (LANE, rows)))
    copies = []
    for which in range(views):
        margin = early_ref.at[which] if which < EARLY else late_ref.at[which - EARLY]

        def put(t, margin_at, lifted_at):
            span = pl.ds(t * SUB, SUB)
            top = tall[which, span, :]
            for j in range(blocks):
                stage[which, span, j * LANE : (j + 1) * LANE] = jnp.maximum(margin_at(j), top - lifted_at(j))

        for end in range(2):
            put(
                end * (tiles - 1),
                lambda j: edge_margin_ref[which, end, j],
                lambda j: edge_ref[which, end, j],
            )

        @pl.loop(1, tiles - 1)
        def _(t):
            put(t, lambda j: margin[t - 1, j], lambda j: lifted_ref[which, t, j])

        copies.append(pltpu.make_async_copy(stage.at[which], out_ref.at[which], sems.at[which]))
        copies[-1].start()
    for copy in copies:
        copy.wait()


def on_device(ty, tx, surface, bearing, disp, altitude):
    rows, cols = surface.shape
    views = bearing.shape[0]
    tiles, blocks = rows // SUB, cols // LANE
    f32 = jnp.float32
    assert tx & (tx - 1) == 0 and tx > 1
    up = lax.ppermute(surface[rows - SUB :], "ty", [(i, (i + 1) % ty) for i in range(ty)])
    down = lax.ppermute(surface[:SUB], "ty", [((i + 1) % ty, i) for i in range(ty)])
    smem = pl.BlockSpec(memory_space=pltpu.SMEM)
    vmem = pl.BlockSpec(memory_space=pltpu.VMEM)
    hbm = pl.BlockSpec(memory_space=pltpu.HBM)
    tile = (SUB, LANE)
    pinned = [pltpu.with_memory_space_constraint(a, pltpu.HBM) for a in (bearing, disp, altitude, surface)]
    lifted, early, edge, peak, terms, shifts = pl.pallas_call(
        functools.partial(inner_kernel, tx=tx),
        out_shape=(
            pltpu.VMEM((views, tiles, blocks) + tile, f32),
            pltpu.VMEM((EARLY, tiles - 2, blocks) + tile, f32),
            pltpu.VMEM((2, blocks, 2 * SUB, LANE), f32),
            pltpu.VMEM((views, tiles) + tile, f32),
            pltpu.VMEM((views, TAPS + 1) + tile, f32),
            pltpu.SMEM((views,), jnp.int32),
        ),
        in_specs=[hbm] * 4,
        out_specs=[vmem] * 5 + [smem],
        scratch_shapes=[
            pltpu.VMEM((blocks, rows, LANE), f32),
            pltpu.VMEM((tiles - 2, blocks) + tile, f32),
            pltpu.SMEM((views,), jnp.int32),
            pltpu.SMEM((views,), jnp.int32),
            pltpu.SMEM((views,), jnp.int32),
            pltpu.SemaphoreType.DMA((blocks,)),
            pltpu.SemaphoreType.DMA((3,)),
        ],
        compiler_params=pltpu.CompilerParams(vmem_limit_bytes=16 * MIB),
        cost_estimate=pl.CostEstimate(flops=views * rows * cols * 40, bytes_accessed=rows * cols * 4, transcendentals=0),
        name="inner",
    )(*pinned)
    outer, peaks = pl.pallas_call(
        functools.partial(edge_kernel, ty=ty),
        out_shape=(pltpu.VMEM((views, 2, blocks) + tile, f32), pltpu.VMEM((views, rows), f32)),
        in_specs=[smem] + [vmem] * 5,
        out_specs=[vmem] * 2,
        scratch_shapes=[pltpu.VMEM((2, blocks, 3 * SUB, LANE), f32), pltpu.VMEM((rows, LANE), f32)],
        compiler_params=pltpu.CompilerParams(vmem_limit_bytes=16 * MIB),
        name="edges",
    )(shifts, terms, up, down, edge, peak)
    partner = lax.ppermute(peaks, "tx", [(i, i ^ 1) for i in range(tx)])
    chip_peaks = jnp.maximum(peaks, partner)
    got = [lax.ppermute(chip_peaks, "tx", [(i, i ^ m) for i in range(tx)]) for m in range(2, tx, 2)]
    late, outer_margin = pl.pallas_call(
        late_kernel,
        out_shape=(
            pltpu.VMEM((views - EARLY, tiles - 2, blocks) + tile, f32),
            pltpu.VMEM((views, 2, blocks) + tile, f32),
        ),
        in_specs=[vmem] * 2,
        out_specs=[vmem] * 2,
        scratch_shapes=[pltpu.VMEM((max(tiles - 2, 2 * views), blocks) + tile, f32)],
        compiler_params=pltpu.CompilerParams(vmem_limit_bytes=16 * MIB),
        cost_estimate=pl.CostEstimate(flops=views * rows * cols * 40, bytes_accessed=rows * cols * 4, transcendentals=0),
        name="late",
    )(lifted, outer)
    return pl.pallas_call(
        functools.partial(final_kernel, tx=tx),
        out_shape=jax.ShapeDtypeStruct((views, rows, cols), f32),
        in_specs=[vmem] * (tx // 2 + 5),
        out_specs=hbm,
        scratch_shapes=[
            pltpu.VMEM((views, rows, cols), f32),
            pltpu.VMEM((views, rows, LANE), f32),
            pltpu.SemaphoreType.DMA((views,)),
        ],
        compiler_params=pltpu.CompilerParams(vmem_limit_bytes=16 * MIB),
        name="finish",
    )(partner, *got, lifted, early, late, outer, outer_margin)


def solution(mesh):
    return jax.shard_map(
        functools.partial(on_device, mesh.shape["ty"], mesh.shape["tx"]),
        mesh=mesh,
        in_specs=(P("ty", "tx"), P(), P(), P()),
        out_specs=P(None, "ty", "tx"),
        check_vma=False,
    )
```

```python
import functools
import math

import jax
import jax.numpy as jnp
from jax import lax
from jax.experimental import pallas as pl
from jax.experimental.pallas import tpu as pltpu
from jax.sharding import PartitionSpec as P

TAPS = 4
SUB = 8
LANE = 128
MIB = 1 << 20
DELAY = 2


def view_terms(bearing_ref, class_ref, which, easting_span):
    bearing = bearing_ref[which]
    frac = (lax.rem(bearing * 5, 16).astype(jnp.float32) + 0.5) * 0.0625
    theta = (bearing.astype(jnp.float32) - 7.5) * (math.pi / 32.0)
    stride = 1.0 / jnp.cos(jnp.full((SUB, LANE), theta, jnp.float32))
    slope = (1.0 + class_ref[which].astype(jnp.float32)) * (1.0 / (4.0 * easting_span))
    cube = frac * frac * frac
    square = frac * frac
    weights = (
        (-cube + 2.0 * square - frac) * 0.5,
        (3.0 * cube - 5.0 * square + 2.0) * 0.5,
        (-3.0 * cube + 4.0 * square + frac) * 0.5,
        (cube - square) * 0.5,
    )
    return weights, stride * slope


def column_tile(first_col, block):
    lane = lax.broadcasted_iota(jnp.int32, (SUB, LANE), 1)
    return (lane + (first_col + block * LANE)).astype(jnp.float32)


def lifted_tile(weights, ramp, rows_at):
    total = weights[0] * rows_at(0)
    for tap in range(1, TAPS):
        total = total + weights[tap] * rows_at(tap)
    return total + ramp


def windows(tiles, carried):
    sub = lax.broadcasted_iota(jnp.int32, tiles[0].shape, 0)
    step = 1
    while step < SUB:
        here = [pltpu.roll(tile, step, 0) for tile in tiles]
        left = [carried[step]] + here[:-1]
        carried[step] = here[-1]
        tiles = [jnp.maximum(v, jnp.where(sub < step, p, q)) for v, p, q in zip(tiles, left, here)]
        step *= 2
    return tiles


def inner_kernel(
    bearing_hbm, disp_hbm, class_hbm, x_ref, lifted_ref, edge_ref, peak_ref, terms_ref, disp_out,
    own, bearing_ref, disp_ref, class_ref, sems, few_sems, *, tx,
):
    rows, cols = x_ref.shape
    blocks, tiles = cols // LANE, rows // SUB
    views = bearing_ref.shape[0]
    few = [
        pltpu.make_async_copy(source, target, few_sems.at[i])
        for i, (source, target) in enumerate(((bearing_hbm, bearing_ref), (disp_hbm, disp_ref), (class_hbm, class_ref)))
    ]
    for copy in few:
        copy.start()

    def block_copy(j):
        return pltpu.make_async_copy(x_ref.at[:, pl.ds(pl.multiple_of(j * LANE, LANE), LANE)], own.at[j], sems.at[j])

    for j in range(blocks):
        block_copy(j).start()
    first_col = lax.axis_index("tx") * cols
    for copy in few:
        copy.wait()
    for which in range(views):
        weights, rise = view_terms(bearing_ref, class_ref, which, cols * tx)
        disp_out[which] = disp_ref[which]
        for tap in range(TAPS):
            terms_ref[which, tap] = jnp.full((SUB, LANE), weights[tap], jnp.float32)
        terms_ref[which, TAPS] = rise
        for t in range(1, tiles - 1):
            peak_ref[which, t] = jnp.full((SUB, LANE), -jnp.inf, jnp.float32)

    @pl.loop(0, blocks)
    def _(j):
        block_copy(j).wait()
        edge_ref[0, j] = own[j, 0 : 2 * SUB, :]
        edge_ref[1, j] = own[j, rows - 2 * SUB : rows, :]
        column = column_tile(first_col, j)
        for which in range(views):
            weights = [terms_ref[which, tap] for tap in range(TAPS)]
            ramp = terms_ref[which, TAPS] * column
            disp = disp_ref[which] - 1
            for t in range(1, tiles - 1):
                value = lifted_tile(weights, ramp, lambda tap: own[j, pl.ds(t * SUB + disp + tap, SUB), :])
                lifted_ref[which, j, t * SUB : (t + 1) * SUB, :] = value
                peak_ref[which, t] = jnp.maximum(peak_ref[which, t], value)


def edge_kernel(disp_ref, terms_ref, up_ref, down_ref, edge_ref, peak_ref, inner_ref, lifted_ref, sent_ref, ring, tall, *, ty):
    cols = up_ref.shape[1]
    blocks = cols // LANE
    views, tiles = peak_ref.shape[:2]
    place = lax.axis_index("ty")
    first_col = lax.axis_index("tx") * cols
    for j in range(blocks):
        span = slice(j * LANE, (j + 1) * LANE)
        ring[0, j, 0:SUB, :] = jnp.where(place == 0, 0.0, up_ref[:, span])
        ring[0, j, SUB : 3 * SUB, :] = edge_ref[0, j]
        ring[1, j, 0 : 2 * SUB, :] = edge_ref[1, j]
        ring[1, j, 2 * SUB : 3 * SUB, :] = jnp.where(place == ty - 1, 0.0, down_ref[:, span])
    for which in range(views):
        weights, rise = [terms_ref[which, tap] for tap in range(TAPS)], terms_ref[which, TAPS]
        disp = disp_ref[which] - 1
        tops = []
        for end in range(2):
            top = None
            for j in range(blocks):
                value = lifted_tile(
                    weights,
                    rise * column_tile(first_col, j),
                    lambda tap: ring[end, j, pl.ds(SUB + disp + tap, SUB), :],
                )
                first = end * (tiles - 1) * SUB
                lifted_ref[which, j, first : first + SUB, :] = value
                top = value if top is None else jnp.maximum(top, value)
            tops.append(top)
        tall[0:SUB, :] = tops[0]
        for t in range(1, tiles - 1):
            tall[t * SUB : (t + 1) * SUB, :] = peak_ref[which, t]
        tall[(tiles - 1) * SUB : tiles * SUB, :] = tops[1]
        sent_ref[which : which + 1, :] = jnp.max(jnp.transpose(tall[...]), axis=0, keepdims=True)


def late_kernel(lifted_ref, margin_ref, turned, back):
    views, blocks, rows = lifted_ref.shape[:3]
    units = [(which, j) for which in range(views) for j in range(blocks)]
    lowest = jnp.full((SUB, rows), -jnp.inf, jnp.float32)
    carried = {}
    for n in range(len(units) + 2 * DELAY):
        if n < len(units):
            which, j = units[n]
            turned[which, j] = jnp.transpose(lifted_ref[which, j])
        if DELAY <= n < len(units) + DELAY:
            which, j = units[n - DELAY]
            if j == 0:
                carried = {1: lowest, 2: lowest, 4: lowest}
                peak = lowest
            tiles = [turned[which, j, i : i + SUB, :] for i in range(0, LANE, SUB)]
            for i, tile in enumerate(windows(tiles, carried)):
                peak = jnp.maximum(peak, tile)
                back[which, j, i * SUB : (i + 1) * SUB, :] = peak - tiles[i]
        if 2 * DELAY <= n:
            which, j = units[n - 2 * DELAY]
            margin_ref[which, j] = jnp.transpose(back[which, j])


def final_kernel(*refs, tx):
    partner_ref, *got_refs = refs[: tx // 2]
    lifted_ref, margin_ref, out_ref, stage, tall, sems = refs[tx // 2 :]
    views, rows, cols = out_ref.shape
    blocks, tiles = cols // LANE, rows // SUB
    place = lax.axis_index("tx")
    chip = place // 2
    before = jnp.where(lax.rem(place, 2) == 1, partner_ref[...], -jnp.inf)
    for i, got_ref in enumerate(got_refs):
        before = jnp.maximum(before, jnp.where((chip ^ (i + 1)) < chip, got_ref[...], -jnp.inf))
    for which in range(views):
        tall[which] = jnp.transpose(jnp.broadcast_to(before[which : which + 1, :], (LANE, rows)))
    copies = []
    for which in range(views):

        @pl.loop(0, tiles)
        def _(t):
            span = pl.ds(t * SUB, SUB)
            top = tall[which, span, :]
            for j in range(blocks):
                stage[which, span, j * LANE : (j + 1) * LANE] = jnp.maximum(
                    margin_ref[which, j, span, :], top - lifted_ref[which, j, span, :]
                )

        copies.append(pltpu.make_async_copy(stage.at[which], out_ref.at[which], sems.at[which]))
        copies[-1].start()
    for copy in copies:
        copy.wait()


def on_device(ty, tx, surface, bearing, disp, altitude):
    rows, cols = surface.shape
    views = bearing.shape[0]
    tiles, blocks = rows // SUB, cols // LANE
    f32 = jnp.float32
    assert tx & (tx - 1) == 0 and tx > 1
    up = lax.ppermute(surface[rows - SUB :], "ty", [(i, (i + 1) % ty) for i in range(ty)])
    down = lax.ppermute(surface[:SUB], "ty", [((i + 1) % ty, i) for i in range(ty)])
    smem = pl.BlockSpec(memory_space=pltpu.SMEM)
    vmem = pl.BlockSpec(memory_space=pltpu.VMEM)
    hbm = pl.BlockSpec(memory_space=pltpu.HBM)
    tile = (SUB, LANE)
    block_shape = (views, blocks, rows, LANE)
    pinned = [pltpu.with_memory_space_constraint(a, pltpu.HBM) for a in (bearing, disp, altitude, surface)]
    lifted, edge, peak, terms, shifts = pl.pallas_call(
        functools.partial(inner_kernel, tx=tx),
        out_shape=(
            pltpu.VMEM(block_shape, f32),
            pltpu.VMEM((2, blocks, 2 * SUB, LANE), f32),
            pltpu.VMEM((views, tiles) + tile, f32),
            pltpu.VMEM((views, TAPS + 1) + tile, f32),
            pltpu.SMEM((views,), jnp.int32),
        ),
        in_specs=[hbm] * 4,
        out_specs=[vmem] * 4 + [smem],
        scratch_shapes=[
            pltpu.VMEM((blocks, rows, LANE), f32),
            pltpu.SMEM((views,), jnp.int32),
            pltpu.SMEM((views,), jnp.int32),
            pltpu.SMEM((views,), jnp.int32),
            pltpu.SemaphoreType.DMA((blocks,)),
            pltpu.SemaphoreType.DMA((3,)),
        ],
        compiler_params=pltpu.CompilerParams(vmem_limit_bytes=16 * MIB),
        cost_estimate=pl.CostEstimate(flops=views * rows * cols * 40, bytes_accessed=rows * cols * 4, transcendentals=0),
        name="inner",
    )(*pinned)
    lifted, peaks = pl.pallas_call(
        functools.partial(edge_kernel, ty=ty),
        out_shape=(pltpu.VMEM(block_shape, f32), pltpu.VMEM((views, rows), f32)),
        in_specs=[smem] + [vmem] * 5 + [pl.BlockSpec(memory_space=pl.ANY)],
        out_specs=[vmem] * 2,
        scratch_shapes=[pltpu.VMEM((2, blocks, 3 * SUB, LANE), f32), pltpu.VMEM((rows, LANE), f32)],
        compiler_params=pltpu.CompilerParams(vmem_limit_bytes=16 * MIB),
        input_output_aliases={6: 0},
        name="edges",
    )(shifts, terms, up, down, edge, peak, lifted)
    partner = lax.ppermute(peaks, "tx", [(i, i ^ 1) for i in range(tx)])
    chip_peaks = jnp.maximum(peaks, partner)
    got = [lax.ppermute(chip_peaks, "tx", [(i, i ^ m) for i in range(tx)]) for m in range(2, tx, 2)]
    margin = pl.pallas_call(
        late_kernel,
        out_shape=pltpu.VMEM(block_shape, f32),
        in_specs=[vmem],
        out_specs=vmem,
        scratch_shapes=[pltpu.VMEM((views, blocks, LANE, rows), f32)] * 2,
        compiler_params=pltpu.CompilerParams(vmem_limit_bytes=24 * MIB),
        cost_estimate=pl.CostEstimate(flops=views * rows * cols * 40, bytes_accessed=rows * cols * 4, transcendentals=0),
        name="late",
    )(lifted)
    return pl.pallas_call(
        functools.partial(final_kernel, tx=tx),
        out_shape=jax.ShapeDtypeStruct((views, rows, cols), f32),
        in_specs=[vmem] * (tx // 2 + 2),
        out_specs=hbm,
        scratch_shapes=[
            pltpu.VMEM((views, rows, cols), f32),
            pltpu.VMEM((views, rows, LANE), f32),
            pltpu.SemaphoreType.DMA((views,)),
        ],
        compiler_params=pltpu.CompilerParams(vmem_limit_bytes=16 * MIB),
        name="finish",
    )(partner, *got, lifted, margin)


def solution(mesh):
    return jax.shard_map(
        functools.partial(on_device, mesh.shape["ty"], mesh.shape["tx"]),
        mesh=mesh,
        in_specs=(P("ty", "tx"), P(), P(), P()),
        out_specs=P(None, "ty", "tx"),
        check_vma=False,
    )
```

```python
import functools
import math

import jax
import jax.numpy as jnp
from jax import lax
from jax.experimental import pallas as pl
from jax.experimental.pallas import tpu as pltpu
from jax.sharding import PartitionSpec as P

TAPS = 4
SUB = 8
LANE = 128
MIB = 1 << 20
REACH = 4
ABOVE, BELOW = REACH + 1, REACH + 2
CHUNKS = 4
DELAY = 2


def view_terms(bearing_ref, class_ref, which, easting_span):
    bearing = bearing_ref[which]
    frac = (lax.rem(bearing * 5, 16).astype(jnp.float32) + 0.5) * 0.0625
    theta = (bearing.astype(jnp.float32) - 7.5) * (math.pi / 32.0)
    stride = 1.0 / jnp.cos(jnp.full((SUB, LANE), theta, jnp.float32))
    slope = (1.0 + class_ref[which].astype(jnp.float32)) * (1.0 / (4.0 * easting_span))
    cube = frac * frac * frac
    square = frac * frac
    weights = (
        (-cube + 2.0 * square - frac) * 0.5,
        (3.0 * cube - 5.0 * square + 2.0) * 0.5,
        (-3.0 * cube + 4.0 * square + frac) * 0.5,
        (cube - square) * 0.5,
    )
    return weights, stride * slope


def column_tile(first_col, block):
    lane = lax.broadcasted_iota(jnp.int32, (SUB, LANE), 1)
    return (lane + (first_col + block * LANE)).astype(jnp.float32)


def lifted_tile(weights, ramp, rows_at):
    total = weights[0] * rows_at(0)
    for tap in range(1, TAPS):
        total = total + weights[tap] * rows_at(tap)
    return total + ramp


def windows(tiles, carried):
    sub = lax.broadcasted_iota(jnp.int32, tiles[0].shape, 0)
    step = 1
    while step < SUB:
        here = [pltpu.roll(tile, step, 0) for tile in tiles]
        left = [carried[step]] + here[:-1]
        carried[step] = here[-1]
        tiles = [jnp.maximum(v, jnp.where(sub < step, p, q)) for v, p, q in zip(tiles, left, here)]
        step *= 2
    return tiles


def prepare_kernel(
    bearing_hbm, disp_hbm, class_hbm, x_ref, tail_ref, head_ref, terms_ref, disp_out,
    ends, bearing_ref, disp_ref, class_ref, end_sems, sems, *, tx,
):
    rows, cols = x_ref.shape
    blocks = cols // LANE
    copies = [
        pltpu.make_async_copy(x_ref.at[pl.ds(first, SUB)], ends.at[end], end_sems.at[end])
        for end, first in enumerate((rows - SUB, 0))
    ] + [
        pltpu.make_async_copy(source, target, sems.at[i])
        for i, (source, target) in enumerate(((bearing_hbm, bearing_ref), (disp_hbm, disp_ref), (class_hbm, class_ref)))
    ]
    for copy in copies:
        copy.start()
    for copy in copies:
        copy.wait()
    for j in range(blocks):
        span = slice(j * LANE, (j + 1) * LANE)
        tail_ref[j * ABOVE : (j + 1) * ABOVE, :] = ends[0, SUB - ABOVE : SUB, span]
        head_ref[j * BELOW : (j + 1) * BELOW, :] = ends[1, 0:BELOW, span]
    for which in range(bearing_ref.shape[0]):
        weights, rise = view_terms(bearing_ref, class_ref, which, cols * tx)
        disp_out[which] = disp_ref[which]
        for tap in range(TAPS):
            terms_ref[which, tap] = jnp.full((SUB, LANE), weights[tap], jnp.float32)
        terms_ref[which, TAPS] = rise


def inner_kernel(disp_ref, terms_ref, x_ref, lifted_ref, edge_ref, peak_ref, own, sems):
    rows, cols = x_ref.shape
    blocks, tiles = cols // LANE, rows // SUB
    views = terms_ref.shape[0]

    def block_copy(j):
        return pltpu.make_async_copy(x_ref.at[:, pl.ds(pl.multiple_of(j * LANE, LANE), LANE)], own.at[j], sems.at[j])

    for j in range(blocks):
        block_copy(j).start()
    first_col = lax.axis_index("tx") * cols
    for which in range(views):
        for t in range(1, tiles - 1):
            peak_ref[which, t] = jnp.full((SUB, LANE), -jnp.inf, jnp.float32)

    @pl.loop(0, blocks)
    def _(j):
        block_copy(j).wait()
        edge_ref[0, j] = own[j, 0 : 2 * SUB, :]
        edge_ref[1, j] = own[j, rows - 2 * SUB : rows, :]
        column = column_tile(first_col, j)
        for which in range(views):
            weights = [terms_ref[which, tap] for tap in range(TAPS)]
            ramp = terms_ref[which, TAPS] * column
            disp = disp_ref[which] - 1
            for t in range(1, tiles - 1):
                value = lifted_tile(weights, ramp, lambda tap: own[j, pl.ds(t * SUB + disp + tap, SUB), :])
                lifted_ref[which, j, t * SUB : (t + 1) * SUB, :] = value
                peak_ref[which, t] = jnp.maximum(peak_ref[which, t], value)


def edge_kernel(disp_ref, terms_ref, up_ref, down_ref, edge_ref, peak_ref, inner_ref, lifted_ref, sent_ref, ring, tall, *, ty):
    blocks = edge_ref.shape[1]
    cols = blocks * LANE
    views, tiles = peak_ref.shape[:2]
    place = lax.axis_index("ty")
    first_col = lax.axis_index("tx") * cols
    for j in range(blocks):
        above = up_ref[j * ABOVE : (j + 1) * ABOVE, :]
        below = down_ref[j * BELOW : (j + 1) * BELOW, :]
        ring[0, j, SUB - ABOVE : SUB, :] = jnp.where(place == 0, 0.0, above)
        ring[0, j, SUB : 3 * SUB, :] = edge_ref[0, j]
        ring[1, j, 0 : 2 * SUB, :] = edge_ref[1, j]
        ring[1, j, 2 * SUB : 2 * SUB + BELOW, :] = jnp.where(place == ty - 1, 0.0, below)
    for which in range(views):
        weights, rise = [terms_ref[which, tap] for tap in range(TAPS)], terms_ref[which, TAPS]
        disp = disp_ref[which] - 1
        tops = []
        for end in range(2):
            top = None
            for j in range(blocks):
                value = lifted_tile(
                    weights,
                    rise * column_tile(first_col, j),
                    lambda tap: ring[end, j, pl.ds(SUB + disp + tap, SUB), :],
                )
                first = end * (tiles - 1) * SUB
                lifted_ref[which, j, first : first + SUB, :] = value
                top = value if top is None else jnp.maximum(top, value)
            tops.append(top)
        tall[0:SUB, :] = tops[0]
        for t in range(1, tiles - 1):
            tall[t * SUB : (t + 1) * SUB, :] = peak_ref[which, t]
        tall[(tiles - 1) * SUB : tiles * SUB, :] = tops[1]
        sent_ref[which : which + 1, :] = jnp.max(jnp.transpose(tall[...]), axis=0, keepdims=True)


def late_kernel(lifted_ref, margin_ref, turned, back):
    views, blocks, rows = lifted_ref.shape[:3]
    units = [(which, j) for which in range(views) for j in range(blocks)]
    lowest = jnp.full((SUB, rows), -jnp.inf, jnp.float32)
    carried = {}
    for n in range(len(units) + 2 * DELAY):
        if n < len(units):
            which, j = units[n]
            turned[which, j] = jnp.transpose(lifted_ref[which, j])
        if DELAY <= n < len(units) + DELAY:
            which, j = units[n - DELAY]
            if j == 0:
                carried = {1: lowest, 2: lowest, 4: lowest}
                peak = lowest
            tiles = [turned[which, j, i : i + SUB, :] for i in range(0, LANE, SUB)]
            for i, tile in enumerate(windows(tiles, carried)):
                peak = jnp.maximum(peak, tile)
                back[which, j, i * SUB : (i + 1) * SUB, :] = peak - tiles[i]
        if 2 * DELAY <= n:
            which, j = units[n - 2 * DELAY]
            margin_ref[which, j] = jnp.transpose(back[which, j])


def final_kernel(*refs, tx):
    partner_ref, *got_refs = refs[: tx // 2]
    lifted_ref, margin_ref, out_ref, stage, tall, sems = refs[tx // 2 :]
    views, rows, cols = out_ref.shape
    blocks, tiles = cols // LANE, rows // SUB
    place = lax.axis_index("tx")
    chip = place // 2
    before = jnp.where(lax.rem(place, 2) == 1, partner_ref[...], -jnp.inf)
    for i, got_ref in enumerate(got_refs):
        before = jnp.maximum(before, jnp.where((chip ^ (i + 1)) < chip, got_ref[...], -jnp.inf))
    for which in range(views):
        tall[which] = jnp.transpose(jnp.broadcast_to(before[which : which + 1, :], (LANE, rows)))
    chunk = rows // CHUNKS
    copies = []
    for which in range(views):
        for first in range(0, rows, chunk):
            for t in range(first, first + chunk, SUB):
                span = slice(t, t + SUB)
                top = tall[which, span, :]
                for j in range(blocks):
                    stage[which, span, j * LANE : (j + 1) * LANE] = jnp.maximum(
                        margin_ref[which, j, span, :], top - lifted_ref[which, j, span, :]
                    )
            part = pl.ds(first, chunk)
            copies.append(
                pltpu.make_async_copy(stage.at[which, part], out_ref.at[which, part], sems.at[which, first // chunk])
            )
            copies[-1].start()
    for copy in copies:
        copy.wait()


def on_device(ty, tx, surface, bearing, disp, altitude):
    rows, cols = surface.shape
    views = bearing.shape[0]
    tiles, blocks = rows // SUB, cols // LANE
    f32 = jnp.float32
    assert tx & (tx - 1) == 0 and tx > 1
    smem = pl.BlockSpec(memory_space=pltpu.SMEM)
    vmem = pl.BlockSpec(memory_space=pltpu.VMEM)
    hbm = pl.BlockSpec(memory_space=pltpu.HBM)
    tile = (SUB, LANE)
    block_shape = (views, blocks, rows, LANE)
    pinned = [pltpu.with_memory_space_constraint(a, pltpu.HBM) for a in (bearing, disp, altitude, surface)]
    tail, head, terms, shifts = pl.pallas_call(
        functools.partial(prepare_kernel, tx=tx),
        out_shape=(
            pltpu.VMEM((blocks * ABOVE, LANE), f32),
            pltpu.VMEM((blocks * BELOW, LANE), f32),
            pltpu.VMEM((views, TAPS + 1) + tile, f32),
            pltpu.SMEM((views,), jnp.int32),
        ),
        in_specs=[hbm] * 4,
        out_specs=[vmem] * 3 + [smem],
        scratch_shapes=[
            pltpu.VMEM((2, SUB, cols), f32),
            pltpu.SMEM((views,), jnp.int32),
            pltpu.SMEM((views,), jnp.int32),
            pltpu.SMEM((views,), jnp.int32),
            pltpu.SemaphoreType.DMA((2,)),
            pltpu.SemaphoreType.DMA((3,)),
        ],
        compiler_params=pltpu.CompilerParams(vmem_limit_bytes=8 * MIB),
        name="prepare",
    )(*pinned)
    up = lax.ppermute(tail, "ty", [(i, (i + 1) % ty) for i in range(ty)])
    down = lax.ppermute(head, "ty", [((i + 1) % ty, i) for i in range(ty)])
    lifted, edge, peak = pl.pallas_call(
        inner_kernel,
        out_shape=(
            pltpu.VMEM(block_shape, f32),
            pltpu.VMEM((2, blocks, 2 * SUB, LANE), f32),
            pltpu.VMEM((views, tiles) + tile, f32),
        ),
        in_specs=[smem, vmem, hbm],
        out_specs=[vmem] * 3,
        scratch_shapes=[pltpu.VMEM((blocks, rows, LANE), f32), pltpu.SemaphoreType.DMA((blocks,))],
        compiler_params=pltpu.CompilerParams(vmem_limit_bytes=16 * MIB),
        cost_estimate=pl.CostEstimate(flops=views * rows * cols * 40, bytes_accessed=rows * cols * 4, transcendentals=0),
        name="inner",
    )(shifts, terms, pinned[3])
    lifted, peaks = pl.pallas_call(
        functools.partial(edge_kernel, ty=ty),
        out_shape=(pltpu.VMEM(block_shape, f32), pltpu.VMEM((views, rows), f32)),
        in_specs=[smem] + [vmem] * 5 + [pl.BlockSpec(memory_space=pl.ANY)],
        out_specs=[vmem] * 2,
        scratch_shapes=[pltpu.VMEM((2, blocks, 3 * SUB, LANE), f32), pltpu.VMEM((rows, LANE), f32)],
        compiler_params=pltpu.CompilerParams(vmem_limit_bytes=16 * MIB),
        input_output_aliases={6: 0},
        name="edges",
    )(shifts, terms, up, down, edge, peak, lifted)
    partner = lax.ppermute(peaks, "tx", [(i, i ^ 1) for i in range(tx)])
    chip_peaks = jnp.maximum(peaks, partner)
    got = [lax.ppermute(chip_peaks, "tx", [(i, i ^ m) for i in range(tx)]) for m in range(2, tx, 2)]
    margin = pl.pallas_call(
        late_kernel,
        out_shape=pltpu.VMEM(block_shape, f32),
        in_specs=[vmem],
        out_specs=vmem,
        scratch_shapes=[pltpu.VMEM((views, blocks, LANE, rows), f32)] * 2,
        compiler_params=pltpu.CompilerParams(vmem_limit_bytes=24 * MIB),
        cost_estimate=pl.CostEstimate(flops=views * rows * cols * 40, bytes_accessed=rows * cols * 4, transcendentals=0),
        name="late",
    )(lifted)
    return pl.pallas_call(
        functools.partial(final_kernel, tx=tx),
        out_shape=jax.ShapeDtypeStruct((views, rows, cols), f32),
        in_specs=[vmem] * (tx // 2 + 2),
        out_specs=hbm,
        scratch_shapes=[
            pltpu.VMEM((views, rows, cols), f32),
            pltpu.VMEM((views, rows, LANE), f32),
            pltpu.SemaphoreType.DMA((views, CHUNKS)),
        ],
        compiler_params=pltpu.CompilerParams(vmem_limit_bytes=16 * MIB),
        name="finish",
    )(partner, *got, lifted, margin)


def solution(mesh):
    return jax.shard_map(
        functools.partial(on_device, mesh.shape["ty"], mesh.shape["tx"]),
        mesh=mesh,
        in_specs=(P("ty", "tx"), P(), P(), P()),
        out_specs=P(None, "ty", "tx"),
        check_vma=False,
    )
```

```python
import functools
import math

import jax
import jax.numpy as jnp
from jax import lax
from jax.experimental import pallas as pl
from jax.experimental.pallas import tpu as pltpu
from jax.sharding import PartitionSpec as P

TAPS = 4
SUB = 8
LANE = 128
MIB = 1 << 20
REACH = 4
BELOW = REACH + 2
CHUNKS = 4
DELAY = 2


def view_terms(bearing_ref, class_ref, which, easting_span):
    bearing = bearing_ref[which]
    frac = (lax.rem(bearing * 5, 16).astype(jnp.float32) + 0.5) * 0.0625
    theta = (bearing.astype(jnp.float32) - 7.5) * (math.pi / 32.0)
    stride = 1.0 / jnp.cos(jnp.full((SUB, LANE), theta, jnp.float32))
    slope = (1.0 + class_ref[which].astype(jnp.float32)) * (1.0 / (4.0 * easting_span))
    cube = frac * frac * frac
    square = frac * frac
    weights = (
        (-cube + 2.0 * square - frac) * 0.5,
        (3.0 * cube - 5.0 * square + 2.0) * 0.5,
        (-3.0 * cube + 4.0 * square + frac) * 0.5,
        (cube - square) * 0.5,
    )
    return weights, stride * slope


def column_tile(first_col, block):
    lane = lax.broadcasted_iota(jnp.int32, (SUB, LANE), 1)
    return (lane + (first_col + block * LANE)).astype(jnp.float32)


def lifted_tile(weights, ramp, rows_at):
    total = weights[0] * rows_at(0)
    for tap in range(1, TAPS):
        total = total + weights[tap] * rows_at(tap)
    return total + ramp


def windows(tiles, carried):
    sub = lax.broadcasted_iota(jnp.int32, tiles[0].shape, 0)
    step = 1
    while step < SUB:
        here = [pltpu.roll(tile, step, 0) for tile in tiles]
        left = [carried[step]] + here[:-1]
        carried[step] = here[-1]
        tiles = [jnp.maximum(v, jnp.where(sub < step, p, q)) for v, p, q in zip(tiles, left, here)]
        step *= 2
    return tiles


def prepare_kernel(
    bearing_hbm, disp_hbm, class_hbm, x_ref, near_ref, far_ref, terms_ref, disp_out,
    ends, bearing_ref, disp_ref, class_ref, end_sems, sems, *, tx,
):
    rows, cols = x_ref.shape
    blocks = cols // LANE
    even = lax.rem(lax.axis_index("ty"), 2) == 0
    copies = [
        pltpu.make_async_copy(x_ref.at[pl.ds(first, SUB)], ends.at[end], end_sems.at[end])
        for end, first in enumerate((rows - SUB, 0))
    ] + [
        pltpu.make_async_copy(source, target, sems.at[i])
        for i, (source, target) in enumerate(((bearing_hbm, bearing_ref), (disp_hbm, disp_ref), (class_hbm, class_ref)))
    ]
    for copy in copies:
        copy.start()
    for copy in copies:
        copy.wait()
    for j in range(blocks):
        span = slice(j * LANE, (j + 1) * LANE)
        tail, head = ends[0, SUB - BELOW : SUB, span], ends[1, 0:BELOW, span]
        near_ref[j * BELOW : (j + 1) * BELOW, :] = jnp.where(even, tail, head)
        far_ref[j * BELOW : (j + 1) * BELOW, :] = jnp.where(even, head, tail)
    for which in range(bearing_ref.shape[0]):
        weights, rise = view_terms(bearing_ref, class_ref, which, cols * tx)
        disp_out[which] = disp_ref[which]
        for tap in range(TAPS):
            terms_ref[which, tap] = jnp.full((SUB, LANE), weights[tap], jnp.float32)
        terms_ref[which, TAPS] = rise


def inner_kernel(disp_ref, terms_ref, x_ref, lifted_ref, edge_ref, peak_ref, own, sems):
    rows, cols = x_ref.shape
    blocks, tiles = cols // LANE, rows // SUB
    views = terms_ref.shape[0]

    def block_copy(j):
        return pltpu.make_async_copy(x_ref.at[:, pl.ds(pl.multiple_of(j * LANE, LANE), LANE)], own.at[j], sems.at[j])

    for j in range(blocks):
        block_copy(j).start()
    first_col = lax.axis_index("tx") * cols
    for which in range(views):
        for t in range(1, tiles - 1):
            peak_ref[which, t] = jnp.full((SUB, LANE), -jnp.inf, jnp.float32)

    @pl.loop(0, blocks)
    def _(j):
        block_copy(j).wait()
        edge_ref[0, j] = own[j, 0 : 2 * SUB, :]
        edge_ref[1, j] = own[j, rows - 2 * SUB : rows, :]
        column = column_tile(first_col, j)
        for which in range(views):
            weights = [terms_ref[which, tap] for tap in range(TAPS)]
            ramp = terms_ref[which, TAPS] * column
            disp = disp_ref[which] - 1
            for t in range(1, tiles - 1):
                value = lifted_tile(weights, ramp, lambda tap: own[j, pl.ds(t * SUB + disp + tap, SUB), :])
                lifted_ref[which, j, t * SUB : (t + 1) * SUB, :] = value
                peak_ref[which, t] = jnp.maximum(peak_ref[which, t], value)


def edge_kernel(disp_ref, terms_ref, near_ref, far_ref, edge_ref, peak_ref, inner_ref, lifted_ref, sent_ref, ring, tall, *, ty):
    blocks = edge_ref.shape[1]
    cols = blocks * LANE
    views, tiles = peak_ref.shape[:2]
    place = lax.axis_index("ty")
    even = lax.rem(place, 2) == 0
    first_col = lax.axis_index("tx") * cols
    for j in range(blocks):
        near, far = near_ref[j * BELOW : (j + 1) * BELOW, :], far_ref[j * BELOW : (j + 1) * BELOW, :]
        above, below = jnp.where(even, far, near), jnp.where(even, near, far)
        ring[0, j, SUB - BELOW : SUB, :] = jnp.where(place == 0, 0.0, above)
        ring[0, j, SUB : 3 * SUB, :] = edge_ref[0, j]
        ring[1, j, 0 : 2 * SUB, :] = edge_ref[1, j]
        ring[1, j, 2 * SUB : 2 * SUB + BELOW, :] = jnp.where(place == ty - 1, 0.0, below)
    for which in range(views):
        weights, rise = [terms_ref[which, tap] for tap in range(TAPS)], terms_ref[which, TAPS]
        disp = disp_ref[which] - 1
        tops = []
        for end in range(2):
            top = None
            for j in range(blocks):
                value = lifted_tile(
                    weights,
                    rise * column_tile(first_col, j),
                    lambda tap: ring[end, j, pl.ds(SUB + disp + tap, SUB), :],
                )
                first = end * (tiles - 1) * SUB
                lifted_ref[which, j, first : first + SUB, :] = value
                top = value if top is None else jnp.maximum(top, value)
            tops.append(top)
        tall[0:SUB, :] = tops[0]
        for t in range(1, tiles - 1):
            tall[t * SUB : (t + 1) * SUB, :] = peak_ref[which, t]
        tall[(tiles - 1) * SUB : tiles * SUB, :] = tops[1]
        sent_ref[which : which + 1, :] = jnp.max(jnp.transpose(tall[...]), axis=0, keepdims=True)


def late_kernel(lifted_ref, margin_ref, turned, back):
    views, blocks, rows = lifted_ref.shape[:3]
    units = [(which, j) for which in range(views) for j in range(blocks)]
    lowest = jnp.full((SUB, rows), -jnp.inf, jnp.float32)
    carried = {}
    for n in range(len(units) + 2 * DELAY):
        if n < len(units):
            which, j = units[n]
            turned[which, j] = jnp.transpose(lifted_ref[which, j])
        if DELAY <= n < len(units) + DELAY:
            which, j = units[n - DELAY]
            if j == 0:
                carried = {1: lowest, 2: lowest, 4: lowest}
                peak = lowest
            tiles = [turned[which, j, i : i + SUB, :] for i in range(0, LANE, SUB)]
            for i, tile in enumerate(windows(tiles, carried)):
                peak = jnp.maximum(peak, tile)
                back[which, j, i * SUB : (i + 1) * SUB, :] = peak - tiles[i]
        if 2 * DELAY <= n:
            which, j = units[n - 2 * DELAY]
            margin_ref[which, j] = jnp.transpose(back[which, j])


def final_kernel(*refs, tx):
    partner_ref, *got_refs = refs[: tx // 2]
    lifted_ref, margin_ref, out_ref, stage, tall, sems = refs[tx // 2 :]
    views, rows, cols = out_ref.shape
    blocks, tiles = cols // LANE, rows // SUB
    place = lax.axis_index("tx")
    chip = place // 2
    before = jnp.where(lax.rem(place, 2) == 1, partner_ref[...], -jnp.inf)
    for i, got_ref in enumerate(got_refs):
        before = jnp.maximum(before, jnp.where((chip ^ (i + 1)) < chip, got_ref[...], -jnp.inf))
    for which in range(views):
        tall[which] = jnp.transpose(jnp.broadcast_to(before[which : which + 1, :], (LANE, rows)))
    chunk = rows // CHUNKS
    copies = []
    for which in range(views):
        for first in range(0, rows, chunk):
            for t in range(first, first + chunk, SUB):
                span = slice(t, t + SUB)
                top = tall[which, span, :]
                for j in range(blocks):
                    stage[which, span, j * LANE : (j + 1) * LANE] = jnp.maximum(
                        margin_ref[which, j, span, :], top - lifted_ref[which, j, span, :]
                    )
            part = pl.ds(first, chunk)
            copies.append(
                pltpu.make_async_copy(stage.at[which, part], out_ref.at[which, part], sems.at[which, first // chunk])
            )
            copies[-1].start()
    for copy in copies:
        copy.wait()


def halo_pairs(ty, tx):
    near, far = [], []
    for row in range(ty):
        for col in range(tx):
            at = row * tx + col
            near.append((at, (row ^ 1) * tx + col))
            other = row - 1 if row % 2 == 0 else row + 1
            far.append((at, other * tx + col if 0 <= other < ty else row * tx + (col ^ 1)))
    return near, far


def on_device(ty, tx, surface, bearing, disp, altitude):
    rows, cols = surface.shape
    views = bearing.shape[0]
    tiles, blocks = rows // SUB, cols // LANE
    f32 = jnp.float32
    assert tx & (tx - 1) == 0 and tx > 1 and ty % 2 == 0
    smem = pl.BlockSpec(memory_space=pltpu.SMEM)
    vmem = pl.BlockSpec(memory_space=pltpu.VMEM)
    hbm = pl.BlockSpec(memory_space=pltpu.HBM)
    tile = (SUB, LANE)
    block_shape = (views, blocks, rows, LANE)
    pinned = [pltpu.with_memory_space_constraint(a, pltpu.HBM) for a in (bearing, disp, altitude, surface)]
    sends_near, sends_far, terms, shifts = pl.pallas_call(
        functools.partial(prepare_kernel, tx=tx),
        out_shape=(
            pltpu.VMEM((blocks * BELOW, LANE), f32),
            pltpu.VMEM((blocks * BELOW, LANE), f32),
            pltpu.VMEM((views, TAPS + 1) + tile, f32),
            pltpu.SMEM((views,), jnp.int32),
        ),
        in_specs=[hbm] * 4,
        out_specs=[vmem] * 3 + [smem],
        scratch_shapes=[
            pltpu.VMEM((2, SUB, cols), f32),
            pltpu.SMEM((views,), jnp.int32),
            pltpu.SMEM((views,), jnp.int32),
            pltpu.SMEM((views,), jnp.int32),
            pltpu.SemaphoreType.DMA((2,)),
            pltpu.SemaphoreType.DMA((3,)),
        ],
        compiler_params=pltpu.CompilerParams(vmem_limit_bytes=8 * MIB),
        name="prepare",
    )(*pinned)
    near, far = halo_pairs(ty, tx)
    got_near = lax.ppermute(sends_near, ("ty", "tx"), near)
    got_far = lax.ppermute(sends_far, ("ty", "tx"), far)
    lifted, edge, peak = pl.pallas_call(
        inner_kernel,
        out_shape=(
            pltpu.VMEM(block_shape, f32),
            pltpu.VMEM((2, blocks, 2 * SUB, LANE), f32),
            pltpu.VMEM((views, tiles) + tile, f32),
        ),
        in_specs=[smem, vmem, hbm],
        out_specs=[vmem] * 3,
        scratch_shapes=[pltpu.VMEM((blocks, rows, LANE), f32), pltpu.SemaphoreType.DMA((blocks,))],
        compiler_params=pltpu.CompilerParams(vmem_limit_bytes=16 * MIB),
        cost_estimate=pl.CostEstimate(flops=views * rows * cols * 40, bytes_accessed=rows * cols * 4, transcendentals=0),
        name="inner",
    )(shifts, terms, pinned[3])
    lifted, peaks = pl.pallas_call(
        functools.partial(edge_kernel, ty=ty),
        out_shape=(pltpu.VMEM(block_shape, f32), pltpu.VMEM((views, rows), f32)),
        in_specs=[smem] + [vmem] * 5 + [pl.BlockSpec(memory_space=pl.ANY)],
        out_specs=[vmem] * 2,
        scratch_shapes=[pltpu.VMEM((2, blocks, 3 * SUB, LANE), f32), pltpu.VMEM((rows, LANE), f32)],
        compiler_params=pltpu.CompilerParams(vmem_limit_bytes=16 * MIB),
        input_output_aliases={6: 0},
        name="edges",
    )(shifts, terms, got_near, got_far, edge, peak, lifted)
    partner = lax.ppermute(peaks, "tx", [(i, i ^ 1) for i in range(tx)])
    chip_peaks = jnp.maximum(peaks, partner)
    got = [lax.ppermute(chip_peaks, "tx", [(i, i ^ m) for i in range(tx)]) for m in range(2, tx, 2)]
    margin = pl.pallas_call(
        late_kernel,
        out_shape=pltpu.VMEM(block_shape, f32),
        in_specs=[vmem],
        out_specs=vmem,
        scratch_shapes=[pltpu.VMEM((views, blocks, LANE, rows), f32)] * 2,
        compiler_params=pltpu.CompilerParams(vmem_limit_bytes=24 * MIB),
        cost_estimate=pl.CostEstimate(flops=views * rows * cols * 40, bytes_accessed=rows * cols * 4, transcendentals=0),
        name="late",
    )(lifted)
    return pl.pallas_call(
        functools.partial(final_kernel, tx=tx),
        out_shape=jax.ShapeDtypeStruct((views, rows, cols), f32),
        in_specs=[vmem] * (tx // 2 + 2),
        out_specs=hbm,
        scratch_shapes=[
            pltpu.VMEM((views, rows, cols), f32),
            pltpu.VMEM((views, rows, LANE), f32),
            pltpu.SemaphoreType.DMA((views, CHUNKS)),
        ],
        compiler_params=pltpu.CompilerParams(vmem_limit_bytes=16 * MIB),
        name="finish",
    )(partner, *got, lifted, margin)


def solution(mesh):
    return jax.shard_map(
        functools.partial(on_device, mesh.shape["ty"], mesh.shape["tx"]),
        mesh=mesh,
        in_specs=(P("ty", "tx"), P(), P(), P()),
        out_specs=P(None, "ty", "tx"),
        check_vma=False,
    )
```

```python
import functools
import math

import jax
import jax.numpy as jnp
from jax import lax
from jax.experimental import pallas as pl
from jax.experimental.pallas import tpu as pltpu
from jax.sharding import PartitionSpec as P

TAPS = 4
SUB = 8
LANE = 128
MIB = 1 << 20
REACH = 4
BELOW = REACH + 2
CHUNKS = 4
DELAY = 2


def view_terms(bearing_ref, class_ref, which, easting_span):
    bearing = bearing_ref[which]
    frac = (lax.rem(bearing * 5, 16).astype(jnp.float32) + 0.5) * 0.0625
    theta = (bearing.astype(jnp.float32) - 7.5) * (math.pi / 32.0)
    stride = 1.0 / jnp.cos(jnp.full((SUB, LANE), theta, jnp.float32))
    slope = (1.0 + class_ref[which].astype(jnp.float32)) * (1.0 / (4.0 * easting_span))
    cube = frac * frac * frac
    square = frac * frac
    weights = (
        (-cube + 2.0 * square - frac) * 0.5,
        (3.0 * cube - 5.0 * square + 2.0) * 0.5,
        (-3.0 * cube + 4.0 * square + frac) * 0.5,
        (cube - square) * 0.5,
    )
    return weights, stride * slope


def column_tile(first_col, block):
    lane = lax.broadcasted_iota(jnp.int32, (SUB, LANE), 1)
    return (lane + (first_col + block * LANE)).astype(jnp.float32)


def lifted_tile(weights, ramp, rows_at):
    total = weights[0] * rows_at(0)
    for tap in range(1, TAPS):
        total = total + weights[tap] * rows_at(tap)
    return total + ramp


def windows(tiles, carried):
    sub = lax.broadcasted_iota(jnp.int32, tiles[0].shape, 0)
    step = 1
    while step < SUB:
        here = [pltpu.roll(tile, step, 0) for tile in tiles]
        left = [carried[step]] + here[:-1]
        carried[step] = here[-1]
        tiles = [jnp.maximum(v, jnp.where(sub < step, p, q)) for v, p, q in zip(tiles, left, here)]
        step *= 2
    return tiles


def prepare_kernel(
    bearing_hbm, disp_hbm, class_hbm, x_ref, near_ref, far_ref, terms_ref, disp_out,
    ends, bearing_ref, disp_ref, class_ref, end_sems, sems, *, tx,
):
    rows, cols = x_ref.shape
    blocks = cols // LANE
    even = lax.rem(lax.axis_index("ty"), 2) == 0
    copies = [
        pltpu.make_async_copy(x_ref.at[pl.ds(first, SUB)], ends.at[end], end_sems.at[end])
        for end, first in enumerate((rows - SUB, 0))
    ] + [
        pltpu.make_async_copy(source, target, sems.at[i])
        for i, (source, target) in enumerate(((bearing_hbm, bearing_ref), (disp_hbm, disp_ref), (class_hbm, class_ref)))
    ]
    for copy in copies:
        copy.start()
    for copy in copies:
        copy.wait()
    for j in range(blocks):
        span = slice(j * LANE, (j + 1) * LANE)
        tail, head = ends[0, SUB - BELOW : SUB, span], ends[1, 0:BELOW, span]
        near_ref[j * BELOW : (j + 1) * BELOW, :] = jnp.where(even, tail, head)
        far_ref[j * BELOW : (j + 1) * BELOW, :] = jnp.where(even, head, tail)
    for which in range(bearing_ref.shape[0]):
        weights, rise = view_terms(bearing_ref, class_ref, which, cols * tx)
        disp_out[which] = disp_ref[which]
        for tap in range(TAPS):
            terms_ref[which, tap] = jnp.full((SUB, LANE), weights[tap], jnp.float32)
        terms_ref[which, TAPS] = rise


def inner_kernel(disp_ref, terms_ref, x_ref, lifted_ref, edge_ref, peak_ref, own, sems):
    rows, cols = x_ref.shape
    blocks, tiles = cols // LANE, rows // SUB
    views = terms_ref.shape[0]

    def block_copy(j):
        return pltpu.make_async_copy(x_ref.at[:, pl.ds(pl.multiple_of(j * LANE, LANE), LANE)], own.at[j], sems.at[j])

    for j in range(blocks):
        block_copy(j).start()
    first_col = lax.axis_index("tx") * cols
    for which in range(views):
        for t in range(1, tiles - 1):
            peak_ref[which, t] = jnp.full((SUB, LANE), -jnp.inf, jnp.float32)

    @pl.loop(0, blocks)
    def _(j):
        block_copy(j).wait()
        edge_ref[0, j] = own[j, 0 : 2 * SUB, :]
        edge_ref[1, j] = own[j, rows - 2 * SUB : rows, :]
        column = column_tile(first_col, j)
        for which in range(views):
            weights = [terms_ref[which, tap] for tap in range(TAPS)]
            ramp = terms_ref[which, TAPS] * column
            disp = disp_ref[which] - 1
            for t in range(1, tiles - 1):
                value = lifted_tile(weights, ramp, lambda tap: own[j, pl.ds(t * SUB + disp + tap, SUB), :])
                lifted_ref[which, j, t * SUB : (t + 1) * SUB, :] = value
                peak_ref[which, t] = jnp.maximum(peak_ref[which, t], value)


def edge_kernel(disp_ref, terms_ref, near_ref, far_ref, edge_ref, peak_ref, inner_ref, lifted_ref, sent_ref, ring, tall, *, ty):
    blocks = edge_ref.shape[1]
    cols = blocks * LANE
    views, tiles = peak_ref.shape[:2]
    place = lax.axis_index("ty")
    even = lax.rem(place, 2) == 0
    first_col = lax.axis_index("tx") * cols
    for j in range(blocks):
        near, far = near_ref[j * BELOW : (j + 1) * BELOW, :], far_ref[j * BELOW : (j + 1) * BELOW, :]
        above, below = jnp.where(even, far, near), jnp.where(even, near, far)
        ring[0, j, SUB - BELOW : SUB, :] = jnp.where(place == 0, 0.0, above)
        ring[0, j, SUB : 3 * SUB, :] = edge_ref[0, j]
        ring[1, j, 0 : 2 * SUB, :] = edge_ref[1, j]
        ring[1, j, 2 * SUB : 2 * SUB + BELOW, :] = jnp.where(place == ty - 1, 0.0, below)
    for which in range(views):
        weights, rise = [terms_ref[which, tap] for tap in range(TAPS)], terms_ref[which, TAPS]
        disp = disp_ref[which] - 1
        tops = []
        for end in range(2):
            top = None
            for j in range(blocks):
                value = lifted_tile(
                    weights,
                    rise * column_tile(first_col, j),
                    lambda tap: ring[end, j, pl.ds(SUB + disp + tap, SUB), :],
                )
                first = end * (tiles - 1) * SUB
                lifted_ref[which, j, first : first + SUB, :] = value
                top = value if top is None else jnp.maximum(top, value)
            tops.append(top)
        tall[0:SUB, :] = tops[0]
        for t in range(1, tiles - 1):
            tall[t * SUB : (t + 1) * SUB, :] = peak_ref[which, t]
        tall[(tiles - 1) * SUB : tiles * SUB, :] = tops[1]
        sent_ref[which : which + 1, :] = jnp.max(jnp.transpose(tall[...]), axis=0, keepdims=True)


def late_kernel(*refs, first_view):
    lifted_ref, margin_ref, turned, back = refs[0], *refs[-3:]
    views, blocks, rows = margin_ref.shape[:3]
    units = [(which, j) for which in range(views) for j in range(blocks)]
    lowest = jnp.full((SUB, rows), -jnp.inf, jnp.float32)
    carried = {}
    for n in range(len(units) + 2 * DELAY):
        if n < len(units):
            which, j = units[n]
            turned[which, j] = jnp.transpose(lifted_ref[first_view + which, j])
        if DELAY <= n < len(units) + DELAY:
            which, j = units[n - DELAY]
            if j == 0:
                carried = {1: lowest, 2: lowest, 4: lowest}
                peak = lowest
            tiles = [turned[which, j, i : i + SUB, :] for i in range(0, LANE, SUB)]
            for i, tile in enumerate(windows(tiles, carried)):
                peak = jnp.maximum(peak, tile)
                back[which, j, i * SUB : (i + 1) * SUB, :] = peak - tiles[i]
        if 2 * DELAY <= n:
            which, j = units[n - 2 * DELAY]
            margin_ref[which, j] = jnp.transpose(back[which, j])


def final_kernel(*refs, tx):
    partner_ref, near_ref, *far_refs = refs[: tx // 2]
    lifted_ref, *margin_refs, out_ref, stage, tall, sems = refs[tx // 2 :]
    views, rows, cols = out_ref.shape
    blocks, tiles = cols // LANE, rows // SUB
    place = lax.axis_index("tx")
    chip, core = place // 2, lax.rem(place, 2)
    before = jnp.where(core == 1, partner_ref[...], -jnp.inf)
    got = [(1, near_ref)]
    for i in range(0, len(far_refs), 2):
        got += [(2 + i + core, far_refs[i]), (3 + i - core, far_refs[i + 1])]
    for offset, got_ref in got:
        before = jnp.maximum(before, jnp.where((chip ^ offset) < chip, got_ref[...], -jnp.inf))
    for which in range(views):
        tall[which] = jnp.transpose(jnp.broadcast_to(before[which : which + 1, :], (LANE, rows)))
    chunk = rows // CHUNKS
    copies = []
    for which in range(views):
        margin_ref = margin_refs[which // (views // len(margin_refs))].at[which % (views // len(margin_refs))]
        for first in range(0, rows, chunk):
            for t in range(first, first + chunk, SUB):
                span = slice(t, t + SUB)
                top = tall[which, span, :]
                for j in range(blocks):
                    stage[which, span, j * LANE : (j + 1) * LANE] = jnp.maximum(
                        margin_ref[j, span, :], top - lifted_ref[which, j, span, :]
                    )
            part = pl.ds(first, chunk)
            copies.append(
                pltpu.make_async_copy(stage.at[which, part], out_ref.at[which, part], sems.at[which, first // chunk])
            )
            copies[-1].start()
    for copy in copies:
        copy.wait()


def halo_pairs(ty, tx):
    near, far = [], []
    for row in range(ty):
        for col in range(tx):
            at = row * tx + col
            near.append((at, (row ^ 1) * tx + col))
            other = row - 1 if row % 2 == 0 else row + 1
            far.append((at, other * tx + col if 0 <= other < ty else row * tx + (col ^ 1)))
    return near, far


def on_device(ty, tx, surface, bearing, disp, altitude):
    rows, cols = surface.shape
    views = bearing.shape[0]
    tiles, blocks = rows // SUB, cols // LANE
    f32 = jnp.float32
    assert tx & (tx - 1) == 0 and tx > 4 and ty % 2 == 0
    smem = pl.BlockSpec(memory_space=pltpu.SMEM)
    vmem = pl.BlockSpec(memory_space=pltpu.VMEM)
    hbm = pl.BlockSpec(memory_space=pltpu.HBM)
    tile = (SUB, LANE)
    block_shape = (views, blocks, rows, LANE)
    pinned = [pltpu.with_memory_space_constraint(a, pltpu.HBM) for a in (bearing, disp, altitude, surface)]
    sends_near, sends_far, terms, shifts = pl.pallas_call(
        functools.partial(prepare_kernel, tx=tx),
        out_shape=(
            pltpu.VMEM((blocks * BELOW, LANE), f32),
            pltpu.VMEM((blocks * BELOW, LANE), f32),
            pltpu.VMEM((views, TAPS + 1) + tile, f32),
            pltpu.SMEM((views,), jnp.int32),
        ),
        in_specs=[hbm] * 4,
        out_specs=[vmem] * 3 + [smem],
        scratch_shapes=[
            pltpu.VMEM((2, SUB, cols), f32),
            pltpu.SMEM((views,), jnp.int32),
            pltpu.SMEM((views,), jnp.int32),
            pltpu.SMEM((views,), jnp.int32),
            pltpu.SemaphoreType.DMA((2,)),
            pltpu.SemaphoreType.DMA((3,)),
        ],
        compiler_params=pltpu.CompilerParams(vmem_limit_bytes=8 * MIB),
        name="prepare",
    )(*pinned)
    near, far = halo_pairs(ty, tx)
    got_near = lax.ppermute(sends_near, ("ty", "tx"), near)
    got_far = lax.ppermute(sends_far, ("ty", "tx"), far)
    lifted, edge, peak = pl.pallas_call(
        inner_kernel,
        out_shape=(
            pltpu.VMEM(block_shape, f32),
            pltpu.VMEM((2, blocks, 2 * SUB, LANE), f32),
            pltpu.VMEM((views, tiles) + tile, f32),
        ),
        in_specs=[smem, vmem, hbm],
        out_specs=[vmem] * 3,
        scratch_shapes=[pltpu.VMEM((blocks, rows, LANE), f32), pltpu.SemaphoreType.DMA((blocks,))],
        compiler_params=pltpu.CompilerParams(vmem_limit_bytes=16 * MIB),
        cost_estimate=pl.CostEstimate(flops=views * rows * cols * 40, bytes_accessed=rows * cols * 4, transcendentals=0),
        name="inner",
    )(shifts, terms, pinned[3])
    lifted, peaks = pl.pallas_call(
        functools.partial(edge_kernel, ty=ty),
        out_shape=(pltpu.VMEM(block_shape, f32), pltpu.VMEM((views, rows), f32)),
        in_specs=[smem] + [vmem] * 5 + [pl.BlockSpec(memory_space=pl.ANY)],
        out_specs=[vmem] * 2,
        scratch_shapes=[pltpu.VMEM((2, blocks, 3 * SUB, LANE), f32), pltpu.VMEM((rows, LANE), f32)],
        compiler_params=pltpu.CompilerParams(vmem_limit_bytes=16 * MIB),
        input_output_aliases={6: 0},
        name="edges",
    )(shifts, terms, got_near, got_far, edge, peak, lifted)
    swap = [(i, i ^ 1) for i in range(tx)]
    partner = lax.ppermute(peaks, "tx", swap)
    chip_peaks = jnp.maximum(peaks, partner)
    far = [
        lax.ppermute(chip_peaks, "tx", [(i, i ^ 2 * (2 * m + i % 2)) for i in range(tx)])
        for m in range(1, tx // 4)
    ]
    near = lax.ppermute(chip_peaks, "tx", [(i, i ^ 2) for i in range(tx)])
    got = [near]
    for part in far:
        got += [part, lax.ppermute(part, "tx", swap)]
    margins = []
    for half in range(2):
        margins.append(
            pl.pallas_call(
                functools.partial(late_kernel, first_view=half * (views // 2)),
                out_shape=pltpu.VMEM((views // 2,) + block_shape[1:], f32),
                in_specs=[vmem] * (1 + half * len(far)),
                out_specs=vmem,
                scratch_shapes=[pltpu.VMEM((views // 2, blocks, LANE, rows), f32)] * 2,
                compiler_params=pltpu.CompilerParams(vmem_limit_bytes=16 * MIB),
                cost_estimate=pl.CostEstimate(flops=views * rows * cols * 20, bytes_accessed=rows * cols * 2, transcendentals=0),
                name="late",
            )(lifted, *far[: half * len(far)])
        )
    return pl.pallas_call(
        functools.partial(final_kernel, tx=tx),
        out_shape=jax.ShapeDtypeStruct((views, rows, cols), f32),
        in_specs=[vmem] * (tx // 2 + 3),
        out_specs=hbm,
        scratch_shapes=[
            pltpu.VMEM((views, rows, cols), f32),
            pltpu.VMEM((views, rows, LANE), f32),
            pltpu.SemaphoreType.DMA((views, CHUNKS)),
        ],
        compiler_params=pltpu.CompilerParams(vmem_limit_bytes=16 * MIB),
        name="finish",
    )(partner, *got, lifted, *margins)


def solution(mesh):
    return jax.shard_map(
        functools.partial(on_device, mesh.shape["ty"], mesh.shape["tx"]),
        mesh=mesh,
        in_specs=(P("ty", "tx"), P(), P(), P()),
        out_specs=P(None, "ty", "tx"),
        check_vma=False,
    )
```
